32 devices in a mesh: gx: 8 (over y, x, core), gy: 4 (over z).
Axes of the slice: x: 2, y: 2, z: 4, core: 2. Of those that a mesh axis runs over, the one named last changes fastest.
Arguments:
- velocity: float32 [2, 320, 1024], P(None, 'gy', 'gx'), may hold values from -4 to 4
- stress: float32 [3, 320, 1024], P(None, 'gy', 'gx'), may hold values from -6 to 6
- wind: float32 [2, 320, 1024], P(None, 'gy', 'gx'), may hold values from -4 to 4
- strength: float32 [320, 1024], P('gy', 'gx'), may hold values from 0.5 to 2
- mass: float32 [320, 1024], P('gy', 'gx'), may hold values from 0.5 to 2
- land_mask: int32 [320, 1024], P('gy', 'gx'), may hold values 0 or 1
- region_mask: int32 [320, 1024], P('gy', 'gx'), may hold values 0 or 1
- observed: float32 [2, 320, 1024], P(None, 'gy', 'gx'), may hold values from -4 to 4
- start_index: int32 [1], replicated, may hold values from 0 to 112
Outputs:
- state_adjoint: float32 [5, 320, 1024], P(None, 'gy', 'gx')
- wind_direction: float32 [2, 320, 1024], P(None, 'gy', 'gx')
The draws below stay inside these ranges and needn't reach their ends.
All inputs are finite; a program needn't handle non-finite values. No bound on the sum of `land_mask` or of `region_mask` on one device may be relied on, other than what follows from the above.
Results may differ from the reference program's by a relative error of at most 0.00002.
Values sent between devices are 32-bit elements; how exact they have to be, the bound alone decides.
A program may use at most 64 MiB of HBM per device.

```python
import math
import jax
import jax.numpy as jnp

STEPS = 8
SUBTOTAL = 120
NY = 320
NX = 1024


def with_ends(result, rng, low, high):
    longest = result.shape.index(max(result.shape))
    spots = []
    for shift in (0, 1):
        where = [jax.random.randint(jax.random.fold_in(rng, axis), (), 0, length) for axis, length in enumerate(result.shape)]
        where[longest] = (where[longest] + shift) % result.shape[longest]
        spots.append(tuple(where))
    return result.at[spots[0]].set(low).at[spots[1]].set(high)


def block_scale(stream_key, extent, pieces, least, top_value):
    gain = 1.0
    for dim, shards_of in pieces:
        heights = jax.random.uniform(jax.random.fold_in(jax.random.fold_in(stream_key, 6), dim), (shards_of,), jnp.float32, least / len(pieces), top_value / len(pieces))
        gain = gain * jnp.repeat(jnp.exp(heights), extent[dim] // shards_of).reshape((-1,) + (1,) * (len(extent) - 1 - dim))
    return gain


def noise(rng, extent, deviation, limit, cuts=(), kind=jnp.bfloat16):
    drawn = deviation * jax.random.normal(rng, extent, jnp.float32)
    if cuts:
        drawn = drawn * block_scale(rng, extent, cuts, -0.22, 0.18)
    return jnp.clip(drawn, -limit, limit).astype(kind)


def setup_inputs(seed: int = 0) -> dict:
    keys = jax.random.split(jax.random.key(seed), 10)
    velocity = noise(keys[0], (2, NY, NX), 0.5, 4.0, ((1, 4), (2, 8)), jnp.float32)
    stress = noise(keys[1], (3, NY, NX), 1.0, 6.0, ((1, 4), (2, 8)), jnp.float32)
    wind = noise(keys[2], (2, NY, NX), 0.5, 4.0, ((1, 4), (2, 8)), jnp.float32)
    strength = jnp.clip(jnp.exp(math.log(2.0) - 1.3862944 * jax.random.uniform(keys[3], (NY, NX), jnp.float32) ** block_scale(keys[3], (NY, NX), ((0, 4), (1, 8)), -0.2, 0.2)), 0.5, 2.0)
    mass = jnp.clip(jnp.exp(math.log(2.0) - 1.3862944 * jax.random.uniform(keys[4], (NY, NX), jnp.float32) ** block_scale(keys[4], (NY, NX), ((0, 4), (1, 8)), -0.2, 0.2)), 0.5, 2.0)
    land_mask = with_ends((jax.random.randint(keys[5], (NY, NX), 0, 10) < 9).astype(jnp.int32), jax.random.fold_in(keys[5], 1), 0, 1)
    region_mask = with_ends((jax.random.randint(keys[6], (NY, NX), 0, 2) < 1).astype(jnp.int32), jax.random.fold_in(keys[6], 1), 0, 1)
    observed = noise(keys[7], (2, NY, NX), 0.5, 4.0, ((1, 4), (2, 8)), jnp.float32)
    start_index = jax.random.randint(keys[8], (1,), 0, SUBTOTAL - STEPS + 1).astype(jnp.int32)
    return dict(velocity=velocity, stress=stress, wind=wind, strength=strength, mass=mass, land_mask=land_mask, region_mask=region_mask, observed=observed, start_index=start_index)


ellipse_sq = 4.0
delta_floor = 0.04
time_step = 0.5
drag_rate = 1.0
norm_eps = 1e-06

def extend(field, signs):
    north = signs[:, None] * field[:, -1, ::-1]
    zero = jnp.zeros_like(field[:, :1, :])
    rows = jnp.concatenate([zero, field, north[:, None, :]], axis=1)
    return jnp.concatenate([rows[:, :, -1:], rows, rows[:, :, :1]], axis=2)

def centred_x(field):
    return 0.5 * (field[1:-1, 2:] - field[1:-1, :-2])

def centred_y(field):
    return 0.5 * (field[2:, 1:-1] - field[:-2, 1:-1])

def stress_update(vel_pad, stress, strength, coef):
    east = vel_pad[0]
    north = vel_pad[1]
    dudx = centred_x(east)
    dudy = centred_y(east)
    dvdx = centred_x(north)
    dvdy = centred_y(north)
    diverge = dudx + dvdy
    tension = dudx - dvdy
    shearing = dudy + dvdx
    delta = jnp.sqrt(diverge * diverge + (tension * tension + shearing * shearing) / ellipse_sq + delta_floor)
    ratio = coef * strength / delta
    denom = 1.0 + coef
    first = (stress[0] + ratio * diverge - coef * strength) / denom
    second = (stress[1] + ratio * tension / ellipse_sq) / denom
    third = (stress[2] + ratio * shearing / ellipse_sq) / denom
    return jnp.stack([first, second, third], axis=0)

def velocity_update(stress_pad, velocity, wind, mass, land):
    first = stress_pad[0]
    second = stress_pad[1]
    third = stress_pad[2]
    force_x = 0.5 * centred_x(first + second) + centred_y(third)
    force_y = 0.5 * centred_y(first - second) + centred_x(third)
    scaled = land / (mass + time_step * drag_rate)
    east = scaled * (mass * velocity[0] + time_step * (force_x + wind[0]))
    north = scaled * (mass * velocity[1] + time_step * (force_y + wind[1]))
    return jnp.stack([east, north], axis=0)

def coefficient(start_index, step):
    return 0.2 + 0.8 * (start_index[0].astype(jnp.float32) + (step + 1)) / SUBTOTAL

def reference(velocity, stress, wind, strength, mass, land_mask, region_mask, observed, start_index):
    land = land_mask.astype(jnp.float32)
    region = region_mask.astype(jnp.float32)
    vel_signs = jnp.array([-1.0, -1.0], dtype=jnp.float32)
    stress_signs = jnp.array([1.0, 1.0, 1.0], dtype=jnp.float32)

    def subcycle(vel, sts, forcing, coef):
        sts = stress_update(extend(vel, vel_signs), sts, strength, coef)
        vel = velocity_update(extend(sts, stress_signs), vel, forcing, mass, land)
        return (vel, sts)
    stepper = jax.checkpoint(subcycle)

    def forward(vel, sts, forcing):
        for step in range(STEPS):
            vel, sts = stepper(vel, sts, forcing, coefficient(start_index, step))
        return vel
    final, pullback = jax.vjp(forward, velocity, stress, wind)
    vel_bar, stress_bar, wind_bar = pullback(region * (final - observed))
    state_adjoint = jnp.concatenate([vel_bar, stress_bar], axis=0)
    spread = jnp.sqrt(jnp.mean(wind_bar * wind_bar) + norm_eps)
    return (state_adjoint, wind_bar / spread)
```

```python
import functools

import jax
import jax.numpy as jnp
from jax import lax
from jax.experimental import pallas as pl
from jax.experimental.pallas import tpu as pltpu
from jax.sharding import PartitionSpec as P

STEPS = 8
SUBTOTAL = 120
HALF = STEPS // 2
HALO = 4 * STEPS
COST_HALO = 2 * STEPS
PAD = 8
NORM_EPS = 1e-06
NF = 13
MESH = pl.DeviceIdType.MESH

U, V, G, M, T, WX, WY, STR, MASS, LAND, REGION, OBU, OBV = range(NF)
A, B8 = MASS, LAND
PH, QH, X1, X2, X3 = OBU, OBV, WX, WY, REGION
SW, SE, NW, NE = range(4)


def groups_of(chunks):
    per = 4
    body = list(range(per, chunks - per))
    mid = [body[i : i + per] for i in range(0, len(body), per)]
    return [list(range(per))] + mid + [list(range(chunks - per, chunks))]


def kernel(
    nx, ny, rows,
    start_ref, vel, sts, wind, strength, mass, land, region, obs,
    state_out, wind_out,
    F, IM, SB, RB, RC, SV, WB, CO, RED1, RED2,
    local_sem, send_sem, recv_sem, red_send, red_recv1, red_recv2,
):
    gx = lax.axis_index("gx")
    gy = lax.axis_index("gy")
    top = gy == ny - 1
    south_most = gy == 0
    lanes = F.shape[3]
    strip = HALO
    per = lanes // strip
    mid = PAD + HALO
    north = mid + rows
    east = lax.rem(gx + 1, nx)
    west = lax.rem(gx + nx - 1, nx)

    barrier = pltpu.get_barrier_semaphore()

    def greet(x, y):
        pl.semaphore_signal(barrier, inc=1, device_id={"gx": x, "gy": y}, device_id_type=MESH)

    for d in range(1, nx):
        greet(lax.rem(gx + d, nx), gy)
    for d in range(1, ny):
        greet(gx, lax.rem(gy + d, ny))

    @pl.when(gy < ny - 1)
    def _():
        greet(east, gy + 1)
        greet(west, gy + 1)

    @pl.when(gy > 0)
    def _():
        greet(east, gy - 1)
        greet(west, gy - 1)

    plan = [
        (vel, U, 2, HALO), (sts, G, 3, HALO), (wind, WX, 2, HALO), (strength, STR, 0, HALO),
        (mass, MASS, 0, HALO), (land, 0, -1, HALO), (region, 1, -1, COST_HALO),
        (obs, OBU, 2, COST_HALO),
    ]

    def src_rows(ref, count, first, n):
        return ref.at[:, pl.ds(first, n), :] if count > 0 else ref.at[pl.ds(first, n), :]

    def dst_rows(slot, count, first, n):
        if count > 0:
            return F.at[0, pl.ds(slot, count), pl.ds(first, n), :]
        if count == 0:
            return F.at[0, slot, pl.ds(first, n), :]
        return IM.at[slot, pl.ds(first, n), :]

    locals_ = []
    for i, (ref, slot, count, _) in enumerate(plan):
        copy = pltpu.make_async_copy(
            src_rows(ref, count, 0, rows), dst_rows(slot, count, mid, rows), local_sem.at[i]
        )
        copy.start()
        locals_.append(copy)

    start = start_ref[0].astype(jnp.float32)
    for k in range(STEPS):
        c = 0.2 + 0.8 * (jnp.full((8, lanes), start, jnp.float32) + (k + 1)) / SUBTOTAL
        inv = 1.0 / (1.0 + c)
        CO[k, 0] = inv
        CO[k, 1] = c * inv

    n_plan = len(plan)
    diag = jnp.where(top, 2, 4) - jnp.where(south_most, 2, 0)
    pl.semaphore_wait(barrier, nx - 1 + ny - 1 + diag)

    up_x = jnp.where(top, nx - 1 - gx, gx)
    up_y = jnp.where(top, gy, gy + 1)
    up_row = jnp.where(top, north, PAD)
    up_copies, down_copies = [], []
    for i, (ref, slot, count, width) in enumerate(plan):
        first = pl.multiple_of(up_row + (HALO - width), 8)
        up_copies.append(pltpu.make_async_remote_copy(
            src_ref=src_rows(ref, count, rows - width, width),
            dst_ref=dst_rows(slot, count, first, width),
            send_sem=send_sem.at[i],
            recv_sem=recv_sem.at[jnp.where(top, n_plan + i, i)],
            device_id={"gx": up_x, "gy": up_y}, device_id_type=MESH,
        ))
        down_copies.append(pltpu.make_async_remote_copy(
            src_ref=src_rows(ref, count, 0, width),
            dst_ref=dst_rows(slot, count, north, width),
            send_sem=send_sem.at[n_plan + i],
            recv_sem=recv_sem.at[n_plan + i],
            device_id={"gx": gx, "gy": jnp.maximum(gy - 1, 0)}, device_id_type=MESH,
        ))
    for copy in up_copies:
        copy.start()

    @pl.when(gy > 0)
    def _():
        for copy in down_copies:
            copy.start()

    for copy in locals_:
        copy.wait()

    lane = lax.broadcasted_iota(jnp.int32, (8, lanes), 1)
    part = lane // strip
    is_first = lane == 0
    is_last = lane == lanes - 1
    chunks = rows // 8
    groups = groups_of(chunks)

    def own(f, r):
        if f == LAND:
            return IM[0, pl.ds(r, 8), :].astype(jnp.float32)
        if f == REGION:
            return IM[1, pl.ds(r, 8), :].astype(jnp.float32)
        return F[0, f, pl.ds(r, 8), :]

    def spin(x, shift):
        shift = shift % lanes
        return pltpu.roll(x, shift, 1) if shift else x

    for f in range(NF):
        for g, members in enumerate(groups):
            block = [own(f, mid + 8 * c) for c in members]
            for side in range(2):
                out = None
                for q, x in enumerate(block):
                    y = spin(x, strip * (q + 1) if side == 0 else strip * q)
                    out = y if out is None else jnp.where(part == q, y, out)
                SB[side, f, pl.ds(8 * g, 8), :] = out

    n_groups = len(groups)
    base = 2 * n_plan
    tall = pl.ds(8 * (n_groups - 1), 8)
    short = pl.ds(0, 8)

    def remote(src, dst, s, r, x, y):
        return pltpu.make_async_remote_copy(
            src_ref=src, dst_ref=dst, send_sem=send_sem.at[s], recv_sem=recv_sem.at[r],
            device_id={"gx": x, "gy": y}, device_id_type=MESH,
        )

    side_e = remote(SB.at[0], RB.at[0], base, base, east, gy)
    side_w = remote(SB.at[1], RB.at[1], base + 1, base + 1, west, gy)
    up_ex = jnp.where(top, nx - 1 - east, east)
    up_wx = jnp.where(top, nx - 1 - west, west)
    ce = jnp.where(top, NW, SW)
    cw = jnp.where(top, NE, SE)
    corner_ue = remote(SB.at[0, :, tall, :], RC.at[ce], base + 2, base + 2 + ce, up_ex, up_y)
    corner_uw = remote(SB.at[1, :, tall, :], RC.at[cw], base + 3, base + 2 + cw, up_wx, up_y)
    self_e = pltpu.make_async_copy(SB.at[0, :, tall, :], RC.at[NW], recv_sem.at[base + 2 + NW])
    self_w = pltpu.make_async_copy(SB.at[1, :, tall, :], RC.at[NE], recv_sem.at[base + 2 + NE])
    down_y = jnp.maximum(gy - 1, 0)
    corner_de = remote(SB.at[0, :, short, :], RC.at[NW], base + 4, base + 2 + NW, east, down_y)
    corner_dw = remote(SB.at[1, :, short, :], RC.at[NE], base + 5, base + 2 + NE, west, down_y)
    to_self_e = jnp.logical_and(top, up_ex == gx)
    to_self_w = jnp.logical_and(top, up_wx == gx)

    def either(cond, yes, no):
        pl.when(cond)(yes)
        pl.when(jnp.logical_not(cond))(no)

    side_e.start()
    side_w.start()
    either(to_self_e, self_e.start, corner_ue.start)
    either(to_self_w, self_w.start, corner_uw.start)

    @pl.when(gy > 0)
    def _():
        corner_de.start()
        corner_dw.start()

    side_e.wait_recv()
    side_w.wait_recv()

    def arrived(dst, r):
        remote(dst, dst, 0, r, east, gy).wait_recv()

    @pl.when(gy > 0)
    def _():
        for i, (ref, slot, count, width) in enumerate(plan):
            arrived(dst_rows(slot, count, PAD + HALO - width, width), i)
        arrived(RC.at[SW], base + 2 + SW)
        arrived(RC.at[SE], base + 2 + SE)

    def north_rows(offset):
        for i, (ref, slot, count, width) in enumerate(plan):
            shift = HALO - width if offset else 0
            arrived(dst_rows(slot, count, north + shift, width), n_plan + i)

    either(top, lambda: north_rows(True), lambda: north_rows(False))

    def corner_wait(cond, copy, slot):
        either(cond, copy.wait, lambda: arrived(RC.at[slot], base + 2 + slot))

    corner_wait(to_self_e, self_e, NW)
    corner_wait(to_self_w, self_w, NE)

    for slot, f in ((0, LAND), (1, REGION)):
        for r in range(PAD, north + HALO, 8):
            F[0, f, pl.ds(r, 8), :] = IM[slot, pl.ds(r, 8), :].astype(jnp.float32)

    low = lane < lanes // 2

    def unpack(f, r, q, from_w, from_e):
        F[1, f, pl.ds(r, 8), :] = jnp.where(
            low, spin(from_e, -strip * q), spin(from_w, -strip * (q + 1))
        )

    for f in range(NF):
        for g, members in enumerate(groups):
            from_w = RB[0, f, pl.ds(8 * g, 8), :]
            from_e = RB[1, f, pl.ds(8 * g, 8), :]
            for q, c in enumerate(members):
                unpack(f, mid + 8 * c, q, from_w, from_e)
        for q in range(HALO // 8):
            unpack(f, PAD + 8 * q, q, RC[SW, f], RC[SE, f])
            unpack(f, north + 8 * q, q, RC[NW, f], RC[NE, f])

    @pl.when(south_most)
    def _():
        for col in range(2):
            for f in range(NF):
                for r in range(PAD, mid, 8):
                    F[col, f, pl.ds(r, 8), :] = jnp.zeros((8, lanes), jnp.float32)

    @pl.when(top)
    def _():
        flip_lane = lanes - 1 - lane
        flip_row = 7 - lax.broadcasted_iota(jnp.int32, (8, lanes), 0)

        def flip(x):
            x = jnp.take_along_axis(x, flip_lane, axis=1, mode="promise_in_bounds")
            return jnp.take_along_axis(x, flip_row, axis=0, mode="promise_in_bounds")

        n = HALO // 8
        for col in range(2):
            for f in range(NF):
                sign = -1.0 if f in (U, V, WX, WY, OBU, OBV) else 1.0
                block = [flip(F[col, f, pl.ds(north + 8 * q, 8), :]) for q in range(n)]
                for q in range(n):
                    F[col, f, pl.ds(north + 8 * (n - 1 - q), 8), :] = sign * block[q]

    def load(col, f, r):
        return F[col, f, pl.ds(r, 8), :]

    def save(col, f, r, value):
        F[col, f, pl.ds(r, 8), :] = value

    for r in range(PAD, north + HALO, 8):
        for col in range(2):
            m = load(col, MASS, r)
            scaled = load(col, LAND, r) / (m + 0.5)
            save(col, A, r, scaled * m)
            save(col, B8, r, 0.0625 * scaled)
            quarter = 0.25 * scaled
            save(col, WX, r, quarter * load(col, WX, r))
            save(col, WY, r, quarter * load(col, WY, r))
            save(col, U, r, 0.5 * load(col, U, r))
            save(col, V, r, 0.5 * load(col, V, r))
            s1 = load(col, G, r)
            s2 = load(col, M, r)
            save(col, G, r, 2.0 * (s1 + s2))
            save(col, M, r, 2.0 * (s1 - s2))
            save(col, T, r, 2.0 * load(col, T, r))

    def xdiff(f, r):
        c, e = load(0, f, r), load(1, f, r)
        lo_c = pltpu.roll(jnp.where(is_last, e, c), 1, 1)
        lo_e = pltpu.roll(jnp.where(is_last, c, e), 1, 1)
        hi_c = pltpu.roll(jnp.where(is_first, e, c), lanes - 1, 1)
        hi_e = pltpu.roll(jnp.where(is_first, c, e), lanes - 1, 1)
        return hi_c - lo_c, hi_e - lo_e

    def ydiff(f, r):
        return [load(col, f, r + 1) - load(col, f, r - 1) for col in range(2)]

    sv_lo = PAD + HALO - COST_HALO
    sv_hi = north + COST_HALO

    def forward(k, lo, hi):
        inv, kap = CO[k, 0], CO[k, 1]
        for r in range(lo, hi, 8):
            ux, vx, uy, vy = xdiff(U, r), xdiff(V, r), ydiff(U, r), ydiff(V, r)
            for col in range(2):
                d = ux[col] + vy[col]
                t = ux[col] - vy[col]
                s = uy[col] + vx[col]
                d2 = d + d
                i2 = lax.rsqrt(d2 * d2 + t * t + s * s + 0.16)
                a, b, e = d2 * i2, t * i2, s * i2
                q = kap * load(col, STR, r)
                am = a + a - 2.0
                save(col, G, r, inv * load(col, G, r) + q * (am + b))
                save(col, M, r, inv * load(col, M, r) + q * (am - b))
                save(col, T, r, inv * load(col, T, r) + q * e)
                if sv_lo <= r < sv_hi:
                    at = pl.ds(r - sv_lo, 8)
                    SV[k, col, 0, at, :] = a
                    SV[k, col, 1, at, :] = b
                    SV[k, col, 2, at, :] = e
                    SV[k, col, 3, at, :] = q * i2
        for r in range(lo, hi, 8):
            gxd, txd, td, md = xdiff(G, r), xdiff(T, r), ydiff(T, r), ydiff(M, r)
            for col in range(2):
                a, b = load(col, A, r), load(col, B8, r)
                save(col, U, r, a * load(col, U, r) + load(col, WX, r)
                     + b * (0.5 * gxd[col] + td[col]))
                save(col, V, r, a * load(col, V, r) + load(col, WY, r)
                     + b * (0.5 * md[col] + txd[col]))

    def run(first, count, step):
        def body(i, carry):
            step(first + i)
            return carry
        lax.fori_loop(0, count, body, 0)

    quarter_halo = HALO // 4
    run(0, HALF, lambda k: forward(k, PAD, north + HALO))
    run(HALF, HALF, lambda k: forward(k, PAD + quarter_halo, north + HALO - quarter_halo))

    for r in range(sv_lo, sv_hi, 8):
        for col in range(2):
            reg = load(col, REGION, r)
            b = load(col, B8, r)
            reg2 = reg + reg
            for f, o in ((U, OBU), (V, OBV)):
                x = load(col, f, r)
                bar = reg2 * (x + x - load(col, o, r))
                save(col, f, r, bar)
                save(col, o, r, b * bar)
            for f in (G, M, T):
                save(col, f, r, jnp.zeros((8, lanes), jnp.float32))
    for r in range(0, rows, 8):
        for f in range(2):
            WB[f, pl.ds(r, 8), :] = jnp.zeros((8, lanes), jnp.float32)

    def back_stress(k, lo, hi, count_wind, emit=False):
        inv = CO[k, 0]
        for r in range(lo, hi, 8):
            px, qx, py, qy = xdiff(PH, r), xdiff(QH, r), ydiff(PH, r), ydiff(QH, r)
            if count_wind and mid <= r < north:
                at = pl.ds(r - mid, 8)
                WB[0, at, :] = WB[0, at, :] + load(0, PH, r)
                WB[1, at, :] = WB[1, at, :] + load(0, QH, r)
            for col in range(2):
                at = pl.ds(r - sv_lo, 8)
                a, b, e, w = (SV[k, col, j, at, :] for j in range(4))
                t1 = load(col, G, r) - (px[col] + qy[col])
                t2 = load(col, M, r) - 0.5 * (px[col] - qy[col])
                t3 = load(col, T, r) - (py[col] + qx[col])
                kk = t1 * a + t2 * b + t3 * e
                z = t1 - kk * a
                z2 = z + z
                y2 = t2 - kk * b
                y3 = t3 - kk * e
                save(col, X1, r, w * (z2 + y2))
                save(col, X2, r, w * (z2 - y2))
                save(col, X3, r, w * y3)
                t1, t2, t3 = inv * t1, inv * t2, inv * t3
                if not emit:
                    save(col, G, r, t1)
                    save(col, M, r, t2)
                    save(col, T, r, t3)
                elif col == 0 and mid <= r < north:
                    at = pl.ds(r - mid, 8)
                    state_out[2, at, :] = t1
                    state_out[3, at, :] = t2 + t2
                    state_out[4, at, :] = t3 + t3

    def back_velocity(lo, hi, emit=False):
        for r in range(lo, hi, 8):
            x1, x3, y2, y3 = xdiff(X1, r), xdiff(X3, r), ydiff(X2, r), ydiff(X3, r)
            for col in range(2):
                if emit and col:
                    continue
                a = load(col, A, r)
                ub = a * load(col, U, r) - (x1[col] + y3[col])
                vb = a * load(col, V, r) - (y2[col] + x3[col])
                if emit:
                    at = pl.ds(r - mid, 8)
                    state_out[0, at, :] = 0.5 * ub
                    state_out[1, at, :] = 0.5 * vb
                else:
                    b = load(col, B8, r)
                    save(col, U, r, ub)
                    save(col, V, r, vb)
                    save(col, PH, r, b * ub)
                    save(col, QH, r, b * vb)

    def backward(k, lo, hi):
        back_stress(k, lo, hi, True)
        back_velocity(lo, hi)

    run(0, HALF, lambda i: backward(STEPS - 1 - i, sv_lo, sv_hi))
    near_lo, near_hi = mid - quarter_halo, north + quarter_halo
    run(0, HALF - 1, lambda i: backward(HALF - 1 - i, near_lo, near_hi))

    total = jnp.zeros((8, lanes), jnp.float32)
    for f, p in ((0, PH), (1, QH)):
        for r in range(0, rows, 8):
            at = pl.ds(r, 8)
            w = 4.0 * (WB[f, at, :] + load(0, p, mid + r))
            WB[f, at, :] = w
            total = total + w * w
    RED1[gx] = total
    row_sends = []
    for d in range(1, nx):
        row_sends.append(pltpu.make_async_remote_copy(
            src_ref=RED1.at[gx], dst_ref=RED1.at[gx], send_sem=red_send.at[d],
            recv_sem=red_recv1.at[d],
            device_id={"gx": lax.rem(gx + d, nx), "gy": gy}, device_id_type=MESH,
        ))
    for copy in row_sends:
        copy.start()

    back_stress(0, near_lo, near_hi, False, emit=True)

    def red_wait(ref, sem, d, n, here):
        slot = lax.rem(here + n - d, n)
        pltpu.make_async_remote_copy(
            src_ref=ref.at[slot], dst_ref=ref.at[slot], send_sem=red_send.at[d],
            recv_sem=sem.at[d], device_id={"gx": east, "gy": gy}, device_id_type=MESH,
        ).wait_recv()

    for d in range(1, nx):
        red_wait(RED1, red_recv1, d, nx, gx)
    total = RED1[0]
    for i in range(1, nx):
        total = total + RED1[i]
    RED2[gy] = total
    col_sends = []
    for d in range(1, ny):
        col_sends.append(pltpu.make_async_remote_copy(
            src_ref=RED2.at[gy], dst_ref=RED2.at[gy], send_sem=red_send.at[nx + d],
            recv_sem=red_recv2.at[d],
            device_id={"gx": gx, "gy": lax.rem(gy + d, ny)}, device_id_type=MESH,
        ))
    for copy in col_sends:
        copy.start()

    back_velocity(mid, north, emit=True)

    for d in range(1, ny):
        red_wait(RED2, red_recv2, d, ny, gy)
    total = RED2[0]
    for i in range(1, ny):
        total = total + RED2[i]
    entries = 2 * rows * lanes * nx * ny
    whole = jnp.sum(jnp.sum(total, axis=1, keepdims=True), axis=0, keepdims=True)
    spread = jnp.broadcast_to(whole, (8, lanes)) * (1.0 / entries) + NORM_EPS
    scale = 1.0 / jnp.sqrt(spread)
    for f in range(2):
        for r in range(0, rows, 8):
            at = pl.ds(r, 8)
            wind_out[f, at, :] = WB[f, at, :] * scale

    for copy in row_sends + col_sends + up_copies:
        copy.wait_send()
    side_e.wait_send()
    side_w.wait_send()
    pl.when(jnp.logical_not(to_self_e))(corner_ue.wait_send)
    pl.when(jnp.logical_not(to_self_w))(corner_uw.wait_send)

    @pl.when(gy > 0)
    def _():
        for copy in down_copies:
            copy.wait_send()
        corner_de.wait_send()
        corner_dw.wait_send()


def solution(mesh):
    nx, ny = mesh.shape["gx"], mesh.shape["gy"]

    def per_device(vel, sts, wind, strength, mass, land, region, obs, start):
        rows, lanes = strength.shape
        ext = rows + 2 * HALO + 2 * PAD
        n_groups = len(groups_of(rows // 8))
        f32 = jnp.float32
        hbm = pl.BlockSpec(memory_space=pl.ANY)
        vm = pl.BlockSpec(memory_space=pltpu.VMEM)
        return pl.pallas_call(
            functools.partial(kernel, nx, ny, rows),
            out_shape=(
                jax.ShapeDtypeStruct((5, rows, lanes), f32),
                jax.ShapeDtypeStruct((2, rows, lanes), f32),
            ),
            in_specs=[pl.BlockSpec(memory_space=pltpu.SMEM)] + [hbm] * 8,
            out_specs=(vm, vm),
            scratch_shapes=[
                pltpu.VMEM((2, NF, ext, lanes), f32),
                pltpu.VMEM((2, ext, lanes), jnp.int32),
                pltpu.VMEM((2, NF, 8 * n_groups, lanes), f32),
                pltpu.VMEM((2, NF, 8 * n_groups, lanes), f32),
                pltpu.VMEM((4, NF, 8, lanes), f32),
                pltpu.VMEM((STEPS, 2, 4, rows + 2 * COST_HALO, lanes), f32),
                pltpu.VMEM((2, rows, lanes), f32),
                pltpu.VMEM((STEPS, 2, 8, lanes), f32),
                pltpu.VMEM((nx, 8, lanes), f32),
                pltpu.VMEM((ny, 8, lanes), f32),
                pltpu.SemaphoreType.DMA((8,)),
                pltpu.SemaphoreType.DMA((22,)),
                pltpu.SemaphoreType.DMA((22,)),
                pltpu.SemaphoreType.DMA((nx + ny,)),
                pltpu.SemaphoreType.DMA((nx,)),
                pltpu.SemaphoreType.DMA((ny,)),
            ],
            compiler_params=pltpu.CompilerParams(
                collective_id=0, has_side_effects=True, vmem_limit_bytes=32 * 1024 * 1024
            ),
        )(start, vel, sts, wind, strength, mass, land, region, obs)

    block = P(None, "gy", "gx")
    flat = P("gy", "gx")
    return jax.shard_map(
        per_device,
        mesh=mesh,
        in_specs=(block, block, block, flat, flat, flat, flat, block, P()),
        out_specs=(block, block),
        check_vma=False,
    )
```

```python
import functools

import jax
import jax.numpy as jnp
from jax import lax
from jax.experimental import pallas as pl
from jax.experimental.pallas import tpu as pltpu
from jax.sharding import PartitionSpec as P

STEPS = 8
SUBTOTAL = 120
HALF = STEPS // 2
HALO = 4 * STEPS
COST_HALO = 2 * STEPS
PAD = 8
NORM_EPS = 1e-06
NF = 13
NCRIT = 10
MESH = pl.DeviceIdType.MESH

U, V, G, M, T, WX, WY, STR, MASS, LAND, REGION, OBU, OBV = range(NF)
A, B8 = MASS, LAND
PH, QH, X1, X2, X3 = OBU, OBV, WX, WY, REGION
SW, SE, NW, NE = range(4)


def groups_of(chunks):
    per = 4
    body = list(range(per, chunks - per))
    mid = [body[i : i + per] for i in range(0, len(body), per)]
    return [list(range(per))] + mid + [list(range(chunks - per, chunks))]


def kernel(
    nx, ny, rows,
    start_ref, vel, sts, wind, strength, mass, land, region, obs,
    out,
    F, IM, SB, RB, RC, SV, WB, CO, RED1, RED2,
    local_sem, send_sem, recv_sem, red_send, red_recv1, red_recv2,
):
    gx = lax.axis_index("gx")
    gy = lax.axis_index("gy")
    top = gy == ny - 1
    south_most = gy == 0
    lanes = F.shape[3]
    strip = HALO
    per = lanes // strip
    mid = PAD + HALO
    north = mid + rows
    east = lax.rem(gx + 1, nx)
    west = lax.rem(gx + nx - 1, nx)

    barrier = pltpu.get_barrier_semaphore()

    def greet(x, y):
        pl.semaphore_signal(barrier, inc=1, device_id={"gx": x, "gy": y}, device_id_type=MESH)

    for d in range(1, nx):
        greet(lax.rem(gx + d, nx), gy)
    for d in range(1, ny):
        greet(gx, lax.rem(gy + d, ny))

    @pl.when(gy < ny - 1)
    def _():
        greet(east, gy + 1)
        greet(west, gy + 1)

    @pl.when(gy > 0)
    def _():
        greet(east, gy - 1)
        greet(west, gy - 1)

    plan = [
        (vel, U, 2, HALO), (sts, G, 3, HALO), (wind, WX, 2, HALO), (strength, STR, 0, HALO),
        (mass, MASS, 0, HALO), (land, 0, -1, HALO), (region, 1, -1, COST_HALO),
        (obs, OBU, 2, COST_HALO),
    ]

    def src_rows(ref, count, first, n):
        return ref.at[:, pl.ds(first, n), :] if count > 0 else ref.at[pl.ds(first, n), :]

    def dst_rows(slot, count, first, n):
        if count > 0:
            return F.at[0, pl.ds(slot, count), pl.ds(first, n), :]
        if count == 0:
            return F.at[0, slot, pl.ds(first, n), :]
        return IM.at[slot, pl.ds(first, n), :]

    locals_ = []
    for i, (ref, slot, count, _) in enumerate(plan):
        copy = pltpu.make_async_copy(
            src_rows(ref, count, 0, rows), dst_rows(slot, count, mid, rows), local_sem.at[i]
        )
        copy.start()
        locals_.append(copy)

    start = start_ref[0].astype(jnp.float32)
    for k in range(STEPS):
        c = 0.2 + 0.8 * (jnp.full((8, lanes), start, jnp.float32) + (k + 1)) / SUBTOTAL
        inv = 1.0 / (1.0 + c)
        CO[k, 0] = inv
        CO[k, 1] = c * inv

    n_plan = len(plan)
    diag = jnp.where(top, 2, 4) - jnp.where(south_most, 2, 0)
    pl.semaphore_wait(barrier, nx - 1 + ny - 1 + diag)

    up_x = jnp.where(top, nx - 1 - gx, gx)
    up_y = jnp.where(top, gy, gy + 1)
    up_row = jnp.where(top, north, PAD)
    up_copies, down_copies = [], []
    for i, (ref, slot, count, width) in enumerate(plan):
        first = pl.multiple_of(up_row + (HALO - width), 8)
        up_copies.append(pltpu.make_async_remote_copy(
            src_ref=src_rows(ref, count, rows - width, width),
            dst_ref=dst_rows(slot, count, first, width),
            send_sem=send_sem.at[i],
            recv_sem=recv_sem.at[jnp.where(top, n_plan + i, i)],
            device_id={"gx": up_x, "gy": up_y}, device_id_type=MESH,
        ))
        down_copies.append(pltpu.make_async_remote_copy(
            src_ref=src_rows(ref, count, 0, width),
            dst_ref=dst_rows(slot, count, north, width),
            send_sem=send_sem.at[n_plan + i],
            recv_sem=recv_sem.at[n_plan + i],
            device_id={"gx": gx, "gy": jnp.maximum(gy - 1, 0)}, device_id_type=MESH,
        ))
    late = 6

    def start_rows(lo, hi):
        for copy in up_copies[lo:hi]:
            copy.start()

        @pl.when(gy > 0)
        def _():
            for copy in down_copies[lo:hi]:
                copy.start()

    start_rows(0, late)

    for copy in locals_:
        copy.wait()

    lane = lax.broadcasted_iota(jnp.int32, (8, lanes), 1)
    part = lane // strip
    is_first = lane == 0
    is_last = lane == lanes - 1
    chunks = rows // 8
    groups = groups_of(chunks)

    def own(f, r):
        if f == LAND:
            return IM[0, pl.ds(r, 8), :].astype(jnp.float32)
        if f == REGION:
            return IM[1, pl.ds(r, 8), :].astype(jnp.float32)
        return F[0, f, pl.ds(r, 8), :]

    def spin(x, shift):
        shift = shift % lanes
        return pltpu.roll(x, shift, 1) if shift else x

    for f in range(NF):
        for g, members in enumerate(groups):
            block = [own(f, mid + 8 * c) for c in members]
            for side in range(2):
                packed = None
                for q, x in enumerate(block):
                    y = spin(x, strip * (q + 1) if side == 0 else strip * q)
                    packed = y if packed is None else jnp.where(part == q, y, packed)
                SB[side, f, pl.ds(8 * g, 8), :] = packed

    n_groups = len(groups)
    base = 2 * n_plan
    tall = pl.ds(8 * (n_groups - 1), 8)
    short = pl.ds(0, 8)

    def remote(src, dst, s, r, x, y):
        return pltpu.make_async_remote_copy(
            src_ref=src, dst_ref=dst, send_sem=send_sem.at[s], recv_sem=recv_sem.at[r],
            device_id={"gx": x, "gy": y}, device_id_type=MESH,
        )

    down_y = jnp.maximum(gy - 1, 0)
    up_ex = jnp.where(top, nx - 1 - east, east)
    up_wx = jnp.where(top, nx - 1 - west, west)
    ce = jnp.where(top, NW, SW)
    cw = jnp.where(top, NE, SE)
    to_self_e = jnp.logical_and(top, up_ex == gx)
    to_self_w = jnp.logical_and(top, up_wx == gx)

    def either(cond, yes, no):
        pl.when(cond)(yes)
        pl.when(jnp.logical_not(cond))(no)

    def arrived(dst, r):
        remote(dst, dst, 0, r, east, gy).wait_recv()

    class Edges:
        def __init__(self, f0, n, at):
            fs = pl.ds(f0, n)
            self.fs, self.at = fs, at
            self.side_e = remote(SB.at[0, fs], RB.at[0, fs], at, at, east, gy)
            self.side_w = remote(SB.at[1, fs], RB.at[1, fs], at + 1, at + 1, west, gy)
            hi_e, hi_w = SB.at[0, fs, tall, :], SB.at[1, fs, tall, :]
            lo_e, lo_w = SB.at[0, fs, short, :], SB.at[1, fs, short, :]
            c = at + 2
            self.up_e = remote(hi_e, RC.at[ce, fs], at + 2, c + ce, up_ex, up_y)
            self.up_w = remote(hi_w, RC.at[cw, fs], at + 3, c + cw, up_wx, up_y)
            self.self_e = pltpu.make_async_copy(hi_e, RC.at[NW, fs], recv_sem.at[c + NW])
            self.self_w = pltpu.make_async_copy(hi_w, RC.at[NE, fs], recv_sem.at[c + NE])
            self.down_e = remote(lo_e, RC.at[NW, fs], at + 4, c + NW, east, down_y)
            self.down_w = remote(lo_w, RC.at[NE, fs], at + 5, c + NE, west, down_y)

        def start(self):
            either(to_self_e, self.self_e.start, self.up_e.start)
            either(to_self_w, self.self_w.start, self.up_w.start)

            @pl.when(gy > 0)
            def _():
                self.down_e.start()
                self.down_w.start()

            self.side_e.start()
            self.side_w.start()

        def wait_recv(self):
            c = self.at + 2
            self.side_e.wait_recv()
            self.side_w.wait_recv()

            @pl.when(gy > 0)
            def _():
                arrived(RC.at[SW, self.fs], c + SW)
                arrived(RC.at[SE, self.fs], c + SE)

            either(to_self_e, self.self_e.wait, lambda: arrived(RC.at[NW, self.fs], c + NW))
            either(to_self_w, self.self_w.wait, lambda: arrived(RC.at[NE, self.fs], c + NE))

        def wait_send(self):
            self.side_e.wait_send()
            self.side_w.wait_send()
            pl.when(jnp.logical_not(to_self_e))(self.up_e.wait_send)
            pl.when(jnp.logical_not(to_self_w))(self.up_w.wait_send)

            @pl.when(gy > 0)
            def _():
                self.down_e.wait_send()
                self.down_w.wait_send()

    early_edges = Edges(0, NCRIT, base)
    late_edges = Edges(NCRIT, NF - NCRIT, base + 6)
    early_edges.start()
    start_rows(late, n_plan)
    late_edges.start()

    def wait_rows(lo, hi):
        @pl.when(gy > 0)
        def _():
            for i in range(lo, hi):
                _, slot, count, width = plan[i]
                arrived(dst_rows(slot, count, PAD + HALO - width, width), i)

        def north_rows(folded):
            for i in range(lo, hi):
                _, slot, count, width = plan[i]
                shift = HALO - width if folded else 0
                arrived(dst_rows(slot, count, north + shift, width), n_plan + i)

        either(top, lambda: north_rows(True), lambda: north_rows(False))

    low = lane < lanes // 2

    def unpack(f, r, q, from_w, from_e):
        F[1, f, pl.ds(r, 8), :] = jnp.where(
            low, spin(from_e, -strip * q), spin(from_w, -strip * (q + 1))
        )

    def settle(fields, slot, mask):
        for r in range(PAD, north + HALO, 8):
            F[0, mask, pl.ds(r, 8), :] = IM[slot, pl.ds(r, 8), :].astype(jnp.float32)

        for f in fields:
            for g, members in enumerate(groups):
                from_w = RB[0, f, pl.ds(8 * g, 8), :]
                from_e = RB[1, f, pl.ds(8 * g, 8), :]
                for q, c in enumerate(members):
                    unpack(f, mid + 8 * c, q, from_w, from_e)
            for q in range(HALO // 8):
                unpack(f, PAD + 8 * q, q, RC[SW, f], RC[SE, f])
                unpack(f, north + 8 * q, q, RC[NW, f], RC[NE, f])

        @pl.when(south_most)
        def _():
            for col in range(2):
                for f in fields:
                    for r in range(PAD, mid, 8):
                        F[col, f, pl.ds(r, 8), :] = jnp.zeros((8, lanes), jnp.float32)

        @pl.when(top)
        def _():
            flip_lane = lanes - 1 - lane
            flip_row = 7 - lax.broadcasted_iota(jnp.int32, (8, lanes), 0)

            def flip(x):
                x = jnp.take_along_axis(x, flip_lane, axis=1, mode="promise_in_bounds")
                return jnp.take_along_axis(x, flip_row, axis=0, mode="promise_in_bounds")

            n = HALO // 8
            for col in range(2):
                for f in fields:
                    sign = -1.0 if f in (U, V, WX, WY, OBU, OBV) else 1.0
                    block = [flip(F[col, f, pl.ds(north + 8 * q, 8), :]) for q in range(n)]
                    for q in range(n):
                        F[col, f, pl.ds(north + 8 * (n - 1 - q), 8), :] = sign * block[q]

    early_edges.wait_recv()
    wait_rows(0, late)
    settle(range(NCRIT), 0, LAND)

    def load(col, f, r):
        return F[col, f, pl.ds(r, 8), :]

    def save(col, f, r, value):
        F[col, f, pl.ds(r, 8), :] = value

    for r in range(PAD, north + HALO, 8):
        for col in range(2):
            m = load(col, MASS, r)
            scaled = load(col, LAND, r) / (m + 0.5)
            save(col, A, r, scaled * m)
            save(col, B8, r, 0.0625 * scaled)
            quarter = 0.25 * scaled
            save(col, WX, r, quarter * load(col, WX, r))
            save(col, WY, r, quarter * load(col, WY, r))
            save(col, U, r, 0.5 * load(col, U, r))
            save(col, V, r, 0.5 * load(col, V, r))
            s1 = load(col, G, r)
            s2 = load(col, M, r)
            save(col, G, r, 2.0 * (s1 + s2))
            save(col, M, r, 2.0 * (s1 - s2))
            save(col, T, r, 2.0 * load(col, T, r))

    def xdiff(f, r):
        c, e = load(0, f, r), load(1, f, r)
        lo_c = pltpu.roll(jnp.where(is_last, e, c), 1, 1)
        lo_e = pltpu.roll(jnp.where(is_last, c, e), 1, 1)
        hi_c = pltpu.roll(jnp.where(is_first, e, c), lanes - 1, 1)
        hi_e = pltpu.roll(jnp.where(is_first, c, e), lanes - 1, 1)
        return hi_c - lo_c, hi_e - lo_e

    def ydiff(f, r):
        return [load(col, f, r + 1) - load(col, f, r - 1) for col in range(2)]

    sv_lo = PAD + HALO - COST_HALO
    sv_hi = north + COST_HALO

    def forward(k, lo, hi):
        inv, kap = CO[k, 0], CO[k, 1]
        for r in range(lo, hi, 8):
            ux, vx, uy, vy = xdiff(U, r), xdiff(V, r), ydiff(U, r), ydiff(V, r)
            for col in range(2):
                d = ux[col] + vy[col]
                t = ux[col] - vy[col]
                s = uy[col] + vx[col]
                d2 = d + d
                i2 = lax.rsqrt(d2 * d2 + t * t + s * s + 0.16)
                a, b, e = d2 * i2, t * i2, s * i2
                q = kap * load(col, STR, r)
                am = a + a - 2.0
                save(col, G, r, inv * load(col, G, r) + q * (am + b))
                save(col, M, r, inv * load(col, M, r) + q * (am - b))
                save(col, T, r, inv * load(col, T, r) + q * e)
                if sv_lo <= r < sv_hi:
                    at = pl.ds(r - sv_lo, 8)
                    SV[k, col, 0, at, :] = a
                    SV[k, col, 1, at, :] = b
                    SV[k, col, 2, at, :] = e
                    SV[k, col, 3, at, :] = q * i2
        for r in range(lo, hi, 8):
            gxd, txd, td, md = xdiff(G, r), xdiff(T, r), ydiff(T, r), ydiff(M, r)
            for col in range(2):
                a, b = load(col, A, r), load(col, B8, r)
                save(col, U, r, a * load(col, U, r) + load(col, WX, r)
                     + b * (0.5 * gxd[col] + td[col]))
                save(col, V, r, a * load(col, V, r) + load(col, WY, r)
                     + b * (0.5 * md[col] + txd[col]))

    def run(first, count, step):
        def body(i, carry):
            step(first + i)
            return carry
        lax.fori_loop(0, count, body, 0)

    quarter_halo = HALO // 4
    run(0, HALF, lambda k: forward(k, PAD, north + HALO))
    run(HALF, HALF, lambda k: forward(k, PAD + quarter_halo, north + HALO - quarter_halo))

    late_edges.wait_recv()
    wait_rows(late, n_plan)
    settle(range(NCRIT, NF), 1, REGION)

    for r in range(sv_lo, sv_hi, 8):
        for col in range(2):
            reg = load(col, REGION, r)
            b = load(col, B8, r)
            reg2 = reg + reg
            for f, o in ((U, OBU), (V, OBV)):
                x = load(col, f, r)
                bar = reg2 * (x + x - load(col, o, r))
                save(col, f, r, bar)
                save(col, o, r, b * bar)
            for f in (G, M, T):
                save(col, f, r, jnp.zeros((8, lanes), jnp.float32))
    for r in range(0, rows, 8):
        for f in range(2):
            WB[f, pl.ds(r, 8), :] = jnp.zeros((8, lanes), jnp.float32)

    def back_stress(k, lo, hi, count_wind, emit=False):
        inv = CO[k, 0]
        for r in range(lo, hi, 8):
            px, qx, py, qy = xdiff(PH, r), xdiff(QH, r), ydiff(PH, r), ydiff(QH, r)
            if count_wind and mid <= r < north:
                at = pl.ds(r - mid, 8)
                WB[0, at, :] = WB[0, at, :] + load(0, PH, r)
                WB[1, at, :] = WB[1, at, :] + load(0, QH, r)
            for col in range(2):
                at = pl.ds(r - sv_lo, 8)
                a, b, e, w = (SV[k, col, j, at, :] for j in range(4))
                t1 = load(col, G, r) - (px[col] + qy[col])
                t2 = load(col, M, r) - 0.5 * (px[col] - qy[col])
                t3 = load(col, T, r) - (py[col] + qx[col])
                kk = t1 * a + t2 * b + t3 * e
                z = t1 - kk * a
                z2 = z + z
                y2 = t2 - kk * b
                y3 = t3 - kk * e
                save(col, X1, r, w * (z2 + y2))
                save(col, X2, r, w * (z2 - y2))
                save(col, X3, r, w * y3)
                t1, t2, t3 = inv * t1, inv * t2, inv * t3
                if not emit:
                    save(col, G, r, t1)
                    save(col, M, r, t2)
                    save(col, T, r, t3)
                elif col == 0 and mid <= r < north:
                    at = pl.ds(r - mid, 8)
                    out[2, at, :] = t1
                    out[3, at, :] = t2 + t2
                    out[4, at, :] = t3 + t3

    def back_velocity(lo, hi, emit=False):
        for r in range(lo, hi, 8):
            x1, x3, y2, y3 = xdiff(X1, r), xdiff(X3, r), ydiff(X2, r), ydiff(X3, r)
            for col in range(2):
                if emit and col:
                    continue
                a = load(col, A, r)
                ub = a * load(col, U, r) - (x1[col] + y3[col])
                vb = a * load(col, V, r) - (y2[col] + x3[col])
                if emit:
                    at = pl.ds(r - mid, 8)
                    out[0, at, :] = 0.5 * ub
                    out[1, at, :] = 0.5 * vb
                else:
                    b = load(col, B8, r)
                    save(col, U, r, ub)
                    save(col, V, r, vb)
                    save(col, PH, r, b * ub)
                    save(col, QH, r, b * vb)

    def backward(k, lo, hi):
        back_stress(k, lo, hi, True)
        back_velocity(lo, hi)

    run(0, HALF, lambda i: backward(STEPS - 1 - i, sv_lo, sv_hi))
    near_lo, near_hi = mid - quarter_halo, north + quarter_halo
    run(0, HALF - 1, lambda i: backward(HALF - 1 - i, near_lo, near_hi))

    total = jnp.zeros((8, lanes), jnp.float32)
    for f, p in ((0, PH), (1, QH)):
        for r in range(0, rows, 8):
            at = pl.ds(r, 8)
            w = 4.0 * (WB[f, at, :] + load(0, p, mid + r))
            WB[f, at, :] = w
            total = total + w * w
    total = jnp.sum(total, axis=0, keepdims=True)
    RED1[gx] = total
    row_sends = []
    for d in range(1, nx):
        row_sends.append(pltpu.make_async_remote_copy(
            src_ref=RED1.at[gx], dst_ref=RED1.at[gx], send_sem=red_send.at[d],
            recv_sem=red_recv1.at[d],
            device_id={"gx": lax.rem(gx + d, nx), "gy": gy}, device_id_type=MESH,
        ))
    for copy in row_sends:
        copy.start()

    back_stress(0, near_lo, near_hi, False, emit=True)

    def red_wait(ref, sem, d, n, here):
        slot = lax.rem(here + n - d, n)
        pltpu.make_async_remote_copy(
            src_ref=ref.at[slot], dst_ref=ref.at[slot], send_sem=red_send.at[d],
            recv_sem=sem.at[d], device_id={"gx": east, "gy": gy}, device_id_type=MESH,
        ).wait_recv()

    for d in range(1, nx):
        red_wait(RED1, red_recv1, d, nx, gx)
    total = RED1[0]
    for i in range(1, nx):
        total = total + RED1[i]
    RED2[gy] = total
    col_sends = []
    for d in range(1, ny):
        col_sends.append(pltpu.make_async_remote_copy(
            src_ref=RED2.at[gy], dst_ref=RED2.at[gy], send_sem=red_send.at[nx + d],
            recv_sem=red_recv2.at[d],
            device_id={"gx": gx, "gy": lax.rem(gy + d, ny)}, device_id_type=MESH,
        ))
    for copy in col_sends:
        copy.start()

    back_velocity(mid, north, emit=True)

    for d in range(1, ny):
        red_wait(RED2, red_recv2, d, ny, gy)
    total = RED2[0]
    for i in range(1, ny):
        total = total + RED2[i]
    entries = 2 * rows * lanes * nx * ny
    whole = jnp.sum(total, axis=1, keepdims=True)
    spread = jnp.broadcast_to(whole, (8, lanes)) * (1.0 / entries) + NORM_EPS
    scale = 1.0 / jnp.sqrt(spread)
    for f in range(2):
        for r in range(0, rows, 8):
            at = pl.ds(r, 8)
            out[5 + f, at, :] = WB[f, at, :] * scale

    for copy in row_sends + col_sends + up_copies:
        copy.wait_send()
    early_edges.wait_send()
    late_edges.wait_send()

    @pl.when(gy > 0)
    def _():
        for copy in down_copies:
            copy.wait_send()


def split_kernel(both, state_out, wind_out, sem):
    one = pltpu.make_async_copy(both.at[pl.ds(0, 5)], state_out, sem.at[0])
    two = pltpu.make_async_copy(both.at[pl.ds(5, 2)], wind_out, sem.at[1])
    one.start()
    two.start()
    one.wait()
    two.wait()


def solution(mesh):
    nx, ny = mesh.shape["gx"], mesh.shape["gy"]

    def per_device(vel, sts, wind, strength, mass, land, region, obs, start):
        rows, lanes = strength.shape
        ext = rows + 2 * HALO + 2 * PAD
        n_groups = len(groups_of(rows // 8))
        f32 = jnp.float32
        hbm = pl.BlockSpec(memory_space=pl.ANY)
        vm = pl.BlockSpec(memory_space=pltpu.VMEM)
        vel, sts, wind, strength, mass, land, region, obs = (
            pltpu.with_memory_space_constraint(x, pltpu.HBM)
            for x in (vel, sts, wind, strength, mass, land, region, obs)
        )
        both = pl.pallas_call(
            functools.partial(kernel, nx, ny, rows),
            out_shape=jax.ShapeDtypeStruct((7, rows, lanes), f32),
            in_specs=[pl.BlockSpec(memory_space=pltpu.SMEM)] + [hbm] * 8,
            out_specs=vm,
            scratch_shapes=[
                pltpu.VMEM((2, NF, ext, lanes), f32),
                pltpu.VMEM((2, ext, lanes), jnp.int32),
                pltpu.VMEM((2, NF, 8 * n_groups, lanes), f32),
                pltpu.VMEM((2, NF, 8 * n_groups, lanes), f32),
                pltpu.VMEM((4, NF, 8, lanes), f32),
                pltpu.VMEM((STEPS, 2, 4, rows + 2 * COST_HALO, lanes), f32),
                pltpu.VMEM((2, rows, lanes), f32),
                pltpu.VMEM((STEPS, 2, 8, lanes), f32),
                pltpu.VMEM((nx, 1, lanes), f32),
                pltpu.VMEM((ny, 1, lanes), f32),
                pltpu.SemaphoreType.DMA((8,)),
                pltpu.SemaphoreType.DMA((28,)),
                pltpu.SemaphoreType.DMA((28,)),
                pltpu.SemaphoreType.DMA((nx + ny,)),
                pltpu.SemaphoreType.DMA((nx,)),
                pltpu.SemaphoreType.DMA((ny,)),
            ],
            compiler_params=pltpu.CompilerParams(
                collective_id=0, has_side_effects=True, vmem_limit_bytes=32 * 1024 * 1024
            ),
        )(start, vel, sts, wind, strength, mass, land, region, obs)
        return pl.pallas_call(
            split_kernel,
            out_shape=(
                jax.ShapeDtypeStruct((5, rows, lanes), f32),
                jax.ShapeDtypeStruct((2, rows, lanes), f32),
            ),
            in_specs=[vm],
            out_specs=(hbm, hbm),
            scratch_shapes=[pltpu.SemaphoreType.DMA((2,))],
        )(both)

    block = P(None, "gy", "gx")
    flat = P("gy", "gx")
    return jax.shard_map(
        per_device,
        mesh=mesh,
        in_specs=(block, block, block, flat, flat, flat, flat, block, P()),
        out_specs=(block, block),
        check_vma=False,
    )
```

```python
import functools

import jax
import jax.numpy as jnp
from jax import lax
from jax.experimental import pallas as pl
from jax.experimental.pallas import tpu as pltpu
from jax.sharding import PartitionSpec as P

STEPS = 8
SUBTOTAL = 120
HALF = STEPS // 2
HALO = 4 * STEPS
COST_HALO = 2 * STEPS
PAD = 8
NORM_EPS = 1e-06
NF = 13
NCRIT = 10
MESH = pl.DeviceIdType.MESH

U, V, G, M, T, WX, WY, STR, MASS, LAND, REGION, OBU, OBV = range(NF)
A, B8 = MASS, LAND
PH, QH, X1, X2, X3 = OBU, OBV, WX, WY, REGION
SW, SE, NW, NE = range(4)


def groups_of(chunks):
    per = 4
    body = list(range(per, chunks - per))
    mid = [body[i : i + per] for i in range(0, len(body), per)]
    return [list(range(per))] + mid + [list(range(chunks - per, chunks))]


def kernel(
    nx, ny, rows,
    start_ref, vel, sts, wind, strength, mass, land, region, obs,
    out,
    F, IM, SB, RB, RC, SV, WB, CO, RED1, RED2,
    local_sem, send_sem, recv_sem, red_send, red_recv1, red_recv2,
):
    gx = lax.axis_index("gx")
    gy = lax.axis_index("gy")
    top = gy == ny - 1
    south_most = gy == 0
    lanes = F.shape[3]
    strip = HALO
    per = lanes // strip
    mid = PAD + HALO
    north = mid + rows
    east = lax.rem(gx + 1, nx)
    west = lax.rem(gx + nx - 1, nx)

    barrier = pltpu.get_barrier_semaphore()

    def greet(x, y):
        pl.semaphore_signal(barrier, inc=1, device_id={"gx": x, "gy": y}, device_id_type=MESH)

    for d in range(1, nx):
        greet(lax.rem(gx + d, nx), gy)
    for d in range(1, ny):
        greet(gx, lax.rem(gy + d, ny))

    @pl.when(gy < ny - 1)
    def _():
        greet(east, gy + 1)
        greet(west, gy + 1)

    @pl.when(gy > 0)
    def _():
        greet(east, gy - 1)
        greet(west, gy - 1)

    plan = [
        (vel, U, 2, HALO), (sts, G, 3, HALO), (wind, WX, 2, HALO), (strength, STR, 0, HALO),
        (mass, MASS, 0, HALO), (land, 0, -1, HALO), (region, 1, -1, COST_HALO),
        (obs, OBU, 2, COST_HALO),
    ]

    def src_rows(ref, count, first, n):
        return ref.at[:, pl.ds(first, n), :] if count > 0 else ref.at[pl.ds(first, n), :]

    def dst_rows(slot, count, first, n):
        if count > 0:
            return F.at[0, pl.ds(slot, count), pl.ds(first, n), :]
        if count == 0:
            return F.at[0, slot, pl.ds(first, n), :]
        return IM.at[slot, pl.ds(first, n), :]

    locals_ = []
    for i, (ref, slot, count, _) in enumerate(plan):
        copy = pltpu.make_async_copy(
            src_rows(ref, count, 0, rows), dst_rows(slot, count, mid, rows), local_sem.at[i]
        )
        copy.start()
        locals_.append(copy)

    start = start_ref[0].astype(jnp.float32)
    for k in range(STEPS):
        c = 0.2 + 0.8 * (jnp.full((8, lanes), start, jnp.float32) + (k + 1)) / SUBTOTAL
        inv = 1.0 / (1.0 + c)
        CO[k, 0] = inv
        CO[k, 1] = c * inv

    n_plan = len(plan)
    diag = jnp.where(top, 2, 4) - jnp.where(south_most, 2, 0)
    pl.semaphore_wait(barrier, nx - 1 + ny - 1 + diag)

    up_x = jnp.where(top, nx - 1 - gx, gx)
    up_y = jnp.where(top, gy, gy + 1)
    up_row = jnp.where(top, north, PAD)
    up_copies, down_copies = [], []
    for i, (ref, slot, count, width) in enumerate(plan):
        first = pl.multiple_of(up_row + (HALO - width), 8)
        up_copies.append(pltpu.make_async_remote_copy(
            src_ref=src_rows(ref, count, rows - width, width),
            dst_ref=dst_rows(slot, count, first, width),
            send_sem=send_sem.at[i],
            recv_sem=recv_sem.at[jnp.where(top, n_plan + i, i)],
            device_id={"gx": up_x, "gy": up_y}, device_id_type=MESH,
        ))
        down_copies.append(pltpu.make_async_remote_copy(
            src_ref=src_rows(ref, count, 0, width),
            dst_ref=dst_rows(slot, count, north, width),
            send_sem=send_sem.at[n_plan + i],
            recv_sem=recv_sem.at[n_plan + i],
            device_id={"gx": gx, "gy": jnp.maximum(gy - 1, 0)}, device_id_type=MESH,
        ))
    late = 6

    def start_rows(lo, hi):
        for copy in up_copies[lo:hi]:
            copy.start()

        @pl.when(gy > 0)
        def _():
            for copy in down_copies[lo:hi]:
                copy.start()

    start_rows(0, late)

    for copy in locals_:
        copy.wait()

    lane = lax.broadcasted_iota(jnp.int32, (8, lanes), 1)
    part = lane // strip
    is_first = lane == 0
    is_last = lane == lanes - 1
    chunks = rows // 8
    groups = groups_of(chunks)

    def own(f, r):
        if f == LAND:
            return IM[0, pl.ds(r, 8), :].astype(jnp.float32)
        if f == REGION:
            return IM[1, pl.ds(r, 8), :].astype(jnp.float32)
        return F[0, f, pl.ds(r, 8), :]

    def spin(x, shift):
        shift = shift % lanes
        return pltpu.roll(x, shift, 1) if shift else x

    for f in range(NF):
        for g, members in enumerate(groups):
            block = [own(f, mid + 8 * c) for c in members]
            for side in range(2):
                packed = None
                for q, x in enumerate(block):
                    y = spin(x, strip * (q + 1) if side == 0 else strip * q)
                    packed = y if packed is None else jnp.where(part == q, y, packed)
                SB[side, f, pl.ds(8 * g, 8), :] = packed

    n_groups = len(groups)
    base = 2 * n_plan
    tall = pl.ds(8 * (n_groups - 1), 8)
    short = pl.ds(0, 8)

    def remote(src, dst, s, r, x, y):
        return pltpu.make_async_remote_copy(
            src_ref=src, dst_ref=dst, send_sem=send_sem.at[s], recv_sem=recv_sem.at[r],
            device_id={"gx": x, "gy": y}, device_id_type=MESH,
        )

    down_y = jnp.maximum(gy - 1, 0)
    up_ex = jnp.where(top, nx - 1 - east, east)
    up_wx = jnp.where(top, nx - 1 - west, west)
    ce = jnp.where(top, NW, SW)
    cw = jnp.where(top, NE, SE)
    to_self_e = jnp.logical_and(top, up_ex == gx)
    to_self_w = jnp.logical_and(top, up_wx == gx)

    def either(cond, yes, no):
        pl.when(cond)(yes)
        pl.when(jnp.logical_not(cond))(no)

    def arrived(dst, r):
        remote(dst, dst, 0, r, east, gy).wait_recv()

    class Edges:
        def __init__(self, f0, n, at):
            fs = pl.ds(f0, n)
            self.fs, self.at = fs, at
            self.side_e = remote(SB.at[0, fs], RB.at[0, fs], at, at, east, gy)
            self.side_w = remote(SB.at[1, fs], RB.at[1, fs], at + 1, at + 1, west, gy)
            hi_e, hi_w = SB.at[0, fs, tall, :], SB.at[1, fs, tall, :]
            lo_e, lo_w = SB.at[0, fs, short, :], SB.at[1, fs, short, :]
            c = at + 2
            self.up_e = remote(hi_e, RC.at[ce, fs], at + 2, c + ce, up_ex, up_y)
            self.up_w = remote(hi_w, RC.at[cw, fs], at + 3, c + cw, up_wx, up_y)
            self.self_e = pltpu.make_async_copy(hi_e, RC.at[NW, fs], recv_sem.at[c + NW])
            self.self_w = pltpu.make_async_copy(hi_w, RC.at[NE, fs], recv_sem.at[c + NE])
            self.down_e = remote(lo_e, RC.at[NW, fs], at + 4, c + NW, east, down_y)
            self.down_w = remote(lo_w, RC.at[NE, fs], at + 5, c + NE, west, down_y)

        def start(self):
            either(to_self_e, self.self_e.start, self.up_e.start)
            either(to_self_w, self.self_w.start, self.up_w.start)

            @pl.when(gy > 0)
            def _():
                self.down_e.start()
                self.down_w.start()

            self.side_e.start()
            self.side_w.start()

        def wait_sides(self):
            self.side_e.wait_recv()
            self.side_w.wait_recv()

        def wait_corners(self):
            c = self.at + 2

            @pl.when(gy > 0)
            def _():
                arrived(RC.at[SW, self.fs], c + SW)
                arrived(RC.at[SE, self.fs], c + SE)

            either(to_self_e, self.self_e.wait, lambda: arrived(RC.at[NW, self.fs], c + NW))
            either(to_self_w, self.self_w.wait, lambda: arrived(RC.at[NE, self.fs], c + NE))

        def wait_send(self):
            self.side_e.wait_send()
            self.side_w.wait_send()
            pl.when(jnp.logical_not(to_self_e))(self.up_e.wait_send)
            pl.when(jnp.logical_not(to_self_w))(self.up_w.wait_send)

            @pl.when(gy > 0)
            def _():
                self.down_e.wait_send()
                self.down_w.wait_send()

    early_edges = Edges(0, NCRIT, base)
    late_edges = Edges(NCRIT, NF - NCRIT, base + 6)
    early_edges.start()
    start_rows(late, n_plan)
    late_edges.start()

    def wait_rows(lo, hi):
        @pl.when(gy > 0)
        def _():
            for i in range(lo, hi):
                _, slot, count, width = plan[i]
                arrived(dst_rows(slot, count, PAD + HALO - width, width), i)

        def north_rows(folded):
            for i in range(lo, hi):
                _, slot, count, width = plan[i]
                shift = HALO - width if folded else 0
                arrived(dst_rows(slot, count, north + shift, width), n_plan + i)

        either(top, lambda: north_rows(True), lambda: north_rows(False))

    low = lane < lanes // 2

    def unpack(f, r, q, from_w, from_e):
        F[1, f, pl.ds(r, 8), :] = jnp.where(
            low, spin(from_e, -strip * q), spin(from_w, -strip * (q + 1))
        )

    def mask_rows(slot, mask, lo, hi):
        for r in range(lo, hi, 8):
            F[0, mask, pl.ds(r, 8), :] = IM[slot, pl.ds(r, 8), :].astype(jnp.float32)

    def settle_sides(fields):
        for f in fields:
            for g, members in enumerate(groups):
                from_w = RB[0, f, pl.ds(8 * g, 8), :]
                from_e = RB[1, f, pl.ds(8 * g, 8), :]
                for q, c in enumerate(members):
                    unpack(f, mid + 8 * c, q, from_w, from_e)

    def settle(fields, slot, mask):
        mask_rows(slot, mask, PAD, mid)
        mask_rows(slot, mask, north, north + HALO)

        for f in fields:
            for q in range(HALO // 8):
                unpack(f, PAD + 8 * q, q, RC[SW, f], RC[SE, f])
                unpack(f, north + 8 * q, q, RC[NW, f], RC[NE, f])

        @pl.when(south_most)
        def _():
            for col in range(2):
                for f in fields:
                    for r in range(PAD, mid, 8):
                        F[col, f, pl.ds(r, 8), :] = jnp.zeros((8, lanes), jnp.float32)

        @pl.when(top)
        def _():
            flip_lane = lanes - 1 - lane
            flip_row = 7 - lax.broadcasted_iota(jnp.int32, (8, lanes), 0)

            def flip(x):
                x = jnp.take_along_axis(x, flip_lane, axis=1, mode="promise_in_bounds")
                return jnp.take_along_axis(x, flip_row, axis=0, mode="promise_in_bounds")

            n = HALO // 8
            for col in range(2):
                for f in fields:
                    sign = -1.0 if f in (U, V, WX, WY, OBU, OBV) else 1.0
                    block = [flip(F[col, f, pl.ds(north + 8 * q, 8), :]) for q in range(n)]
                    for q in range(n):
                        F[col, f, pl.ds(north + 8 * (n - 1 - q), 8), :] = sign * block[q]

    def load(col, f, r):
        return F[col, f, pl.ds(r, 8), :]

    def save(col, f, r, value):
        F[col, f, pl.ds(r, 8), :] = value

    def prepare(lo, hi, col):
        for r in range(lo, hi, 8):
            m = load(col, MASS, r)
            scaled = load(col, LAND, r) / (m + 0.5)
            save(col, A, r, scaled * m)
            save(col, B8, r, 0.0625 * scaled)
            quarter = 0.25 * scaled
            save(col, WX, r, quarter * load(col, WX, r))
            save(col, WY, r, quarter * load(col, WY, r))
            save(col, U, r, 0.5 * load(col, U, r))
            save(col, V, r, 0.5 * load(col, V, r))
            s1 = load(col, G, r)
            s2 = load(col, M, r)
            save(col, G, r, 2.0 * (s1 + s2))
            save(col, M, r, 2.0 * (s1 - s2))
            save(col, T, r, 2.0 * load(col, T, r))

    mask_rows(0, LAND, mid, north)
    mask_rows(1, REGION, mid, north)
    prepare(mid, north, 0)
    early_edges.wait_sides()
    settle_sides(range(NCRIT))
    prepare(mid, north, 1)
    early_edges.wait_corners()
    wait_rows(0, late)
    settle(range(NCRIT), 0, LAND)
    for col in range(2):
        prepare(PAD, mid, col)
        prepare(north, north + HALO, col)

    def xdiff(f, r):
        c, e = load(0, f, r), load(1, f, r)
        lo_c = pltpu.roll(jnp.where(is_last, e, c), 1, 1)
        lo_e = pltpu.roll(jnp.where(is_last, c, e), 1, 1)
        hi_c = pltpu.roll(jnp.where(is_first, e, c), lanes - 1, 1)
        hi_e = pltpu.roll(jnp.where(is_first, c, e), lanes - 1, 1)
        return hi_c - lo_c, hi_e - lo_e

    def ydiff(f, r):
        return [load(col, f, r + 1) - load(col, f, r - 1) for col in range(2)]

    sv_lo = PAD + HALO - COST_HALO
    sv_hi = north + COST_HALO

    def forward(k, lo, hi):
        inv, kap = CO[k, 0], CO[k, 1]
        for r in range(lo, hi, 8):
            ux, vx, uy, vy = xdiff(U, r), xdiff(V, r), ydiff(U, r), ydiff(V, r)
            for col in range(2):
                d = ux[col] + vy[col]
                t = ux[col] - vy[col]
                s = uy[col] + vx[col]
                d2 = d + d
                i2 = lax.rsqrt(d2 * d2 + t * t + s * s + 0.16)
                a, b, e = d2 * i2, t * i2, s * i2
                q = kap * load(col, STR, r)
                am = a + a - 2.0
                save(col, G, r, inv * load(col, G, r) + q * (am + b))
                save(col, M, r, inv * load(col, M, r) + q * (am - b))
                save(col, T, r, inv * load(col, T, r) + q * e)
                if sv_lo <= r < sv_hi:
                    at = pl.ds(r - sv_lo, 8)
                    SV[k, col, 0, at, :] = a
                    SV[k, col, 1, at, :] = b
                    SV[k, col, 2, at, :] = e
                    SV[k, col, 3, at, :] = q * i2
        for r in range(lo, hi, 8):
            gxd, txd, td, md = xdiff(G, r), xdiff(T, r), ydiff(T, r), ydiff(M, r)
            for col in range(2):
                a, b = load(col, A, r), load(col, B8, r)
                save(col, U, r, a * load(col, U, r) + load(col, WX, r)
                     + b * (0.5 * gxd[col] + td[col]))
                save(col, V, r, a * load(col, V, r) + load(col, WY, r)
                     + b * (0.5 * md[col] + txd[col]))

    def run(first, count, step):
        def body(i, carry):
            step(first + i)
            return carry
        lax.fori_loop(0, count, body, 0)

    quarter_halo = HALO // 4
    run(0, HALF, lambda k: forward(k, PAD, north + HALO))
    run(HALF, HALF, lambda k: forward(k, PAD + quarter_halo, north + HALO - quarter_halo))

    late_edges.wait_sides()
    late_edges.wait_corners()
    wait_rows(late, n_plan)
    settle_sides(range(NCRIT, NF))
    settle(range(NCRIT, NF), 1, REGION)

    for r in range(sv_lo, sv_hi, 8):
        for col in range(2):
            reg = load(col, REGION, r)
            b = load(col, B8, r)
            reg2 = reg + reg
            for f, o in ((U, OBU), (V, OBV)):
                x = load(col, f, r)
                bar = reg2 * (x + x - load(col, o, r))
                save(col, f, r, bar)
                save(col, o, r, b * bar)
            for f in (G, M, T):
                save(col, f, r, jnp.zeros((8, lanes), jnp.float32))
    for r in range(0, rows, 8):
        for f in range(2):
            WB[f, pl.ds(r, 8), :] = jnp.zeros((8, lanes), jnp.float32)

    def back_stress(k, lo, hi, count_wind, emit=False):
        inv = CO[k, 0]
        for r in range(lo, hi, 8):
            px, qx, py, qy = xdiff(PH, r), xdiff(QH, r), ydiff(PH, r), ydiff(QH, r)
            if count_wind and mid <= r < north:
                at = pl.ds(r - mid, 8)
                WB[0, at, :] = WB[0, at, :] + load(0, PH, r)
                WB[1, at, :] = WB[1, at, :] + load(0, QH, r)
            for col in range(2):
                at = pl.ds(r - sv_lo, 8)
                a, b, e, w = (SV[k, col, j, at, :] for j in range(4))
                t1 = load(col, G, r) - (px[col] + qy[col])
                t2 = load(col, M, r) - 0.5 * (px[col] - qy[col])
                t3 = load(col, T, r) - (py[col] + qx[col])
                kk = t1 * a + t2 * b + t3 * e
                z = t1 - kk * a
                z2 = z + z
                y2 = t2 - kk * b
                y3 = t3 - kk * e
                save(col, X1, r, w * (z2 + y2))
                save(col, X2, r, w * (z2 - y2))
                save(col, X3, r, w * y3)
                t1, t2, t3 = inv * t1, inv * t2, inv * t3
                if not emit:
                    save(col, G, r, t1)
                    save(col, M, r, t2)
                    save(col, T, r, t3)
                elif col == 0 and mid <= r < north:
                    at = pl.ds(r - mid, 8)
                    out[2, at, :] = t1
                    out[3, at, :] = t2 + t2
                    out[4, at, :] = t3 + t3

    def back_velocity(lo, hi, emit=False):
        for r in range(lo, hi, 8):
            x1, x3, y2, y3 = xdiff(X1, r), xdiff(X3, r), ydiff(X2, r), ydiff(X3, r)
            for col in range(2):
                if emit and col:
                    continue
                a = load(col, A, r)
                ub = a * load(col, U, r) - (x1[col] + y3[col])
                vb = a * load(col, V, r) - (y2[col] + x3[col])
                if emit:
                    at = pl.ds(r - mid, 8)
                    out[0, at, :] = 0.5 * ub
                    out[1, at, :] = 0.5 * vb
                else:
                    b = load(col, B8, r)
                    save(col, U, r, ub)
                    save(col, V, r, vb)
                    save(col, PH, r, b * ub)
                    save(col, QH, r, b * vb)

    def backward(k, lo, hi):
        back_stress(k, lo, hi, True)
        back_velocity(lo, hi)

    run(0, HALF, lambda i: backward(STEPS - 1 - i, sv_lo, sv_hi))
    near_lo, near_hi = mid - quarter_halo, north + quarter_halo
    run(0, HALF - 1, lambda i: backward(HALF - 1 - i, near_lo, near_hi))

    total = jnp.zeros((8, lanes), jnp.float32)
    for f, p in ((0, PH), (1, QH)):
        for r in range(0, rows, 8):
            at = pl.ds(r, 8)
            w = 4.0 * (WB[f, at, :] + load(0, p, mid + r))
            WB[f, at, :] = w
            total = total + w * w
    total = jnp.sum(total, axis=0, keepdims=True)
    RED1[gx] = total
    row_sends = []
    for d in range(1, nx):
        row_sends.append(pltpu.make_async_remote_copy(
            src_ref=RED1.at[gx], dst_ref=RED1.at[gx], send_sem=red_send.at[d],
            recv_sem=red_recv1.at[d],
            device_id={"gx": lax.rem(gx + d, nx), "gy": gy}, device_id_type=MESH,
        ))
    for copy in row_sends:
        copy.start()

    back_stress(0, near_lo, near_hi, False, emit=True)

    def red_wait(ref, sem, d, n, here):
        slot = lax.rem(here + n - d, n)
        pltpu.make_async_remote_copy(
            src_ref=ref.at[slot], dst_ref=ref.at[slot], send_sem=red_send.at[d],
            recv_sem=sem.at[d], device_id={"gx": east, "gy": gy}, device_id_type=MESH,
        ).wait_recv()

    for d in range(1, nx):
        red_wait(RED1, red_recv1, d, nx, gx)
    total = RED1[0]
    for i in range(1, nx):
        total = total + RED1[i]
    RED2[gy] = total
    col_sends = []
    for d in range(1, ny):
        col_sends.append(pltpu.make_async_remote_copy(
            src_ref=RED2.at[gy], dst_ref=RED2.at[gy], send_sem=red_send.at[nx + d],
            recv_sem=red_recv2.at[d],
            device_id={"gx": gx, "gy": lax.rem(gy + d, ny)}, device_id_type=MESH,
        ))
    for copy in col_sends:
        copy.start()

    back_velocity(mid, north, emit=True)

    for d in range(1, ny):
        red_wait(RED2, red_recv2, d, ny, gy)
    total = RED2[0]
    for i in range(1, ny):
        total = total + RED2[i]
    entries = 2 * rows * lanes * nx * ny
    whole = jnp.sum(total, axis=1, keepdims=True)
    spread = jnp.broadcast_to(whole, (8, lanes)) * (1.0 / entries) + NORM_EPS
    scale = 1.0 / jnp.sqrt(spread)
    for f in range(2):
        for r in range(0, rows, 8):
            at = pl.ds(r, 8)
            out[5 + f, at, :] = WB[f, at, :] * scale

    for copy in row_sends + col_sends + up_copies:
        copy.wait_send()
    early_edges.wait_send()
    late_edges.wait_send()

    @pl.when(gy > 0)
    def _():
        for copy in down_copies:
            copy.wait_send()


def split_kernel(both, state_out, wind_out, sem):
    one = pltpu.make_async_copy(both.at[pl.ds(0, 5)], state_out, sem.at[0])
    two = pltpu.make_async_copy(both.at[pl.ds(5, 2)], wind_out, sem.at[1])
    one.start()
    two.start()
    one.wait()
    two.wait()


def solution(mesh):
    nx, ny = mesh.shape["gx"], mesh.shape["gy"]

    def per_device(vel, sts, wind, strength, mass, land, region, obs, start):
        rows, lanes = strength.shape
        ext = rows + 2 * HALO + 2 * PAD
        n_groups = len(groups_of(rows // 8))
        f32 = jnp.float32
        hbm = pl.BlockSpec(memory_space=pl.ANY)
        vm = pl.BlockSpec(memory_space=pltpu.VMEM)
        vel, sts, wind, strength, mass, land, region, obs = (
            pltpu.with_memory_space_constraint(x, pltpu.HBM)
            for x in (vel, sts, wind, strength, mass, land, region, obs)
        )
        both = pl.pallas_call(
            functools.partial(kernel, nx, ny, rows),
            out_shape=jax.ShapeDtypeStruct((7, rows, lanes), f32),
            in_specs=[pl.BlockSpec(memory_space=pltpu.SMEM)] + [hbm] * 8,
            out_specs=vm,
            scratch_shapes=[
                pltpu.VMEM((2, NF, ext, lanes), f32),
                pltpu.VMEM((2, ext, lanes), jnp.int32),
                pltpu.VMEM((2, NF, 8 * n_groups, lanes), f32),
                pltpu.VMEM((2, NF, 8 * n_groups, lanes), f32),
                pltpu.VMEM((4, NF, 8, lanes), f32),
                pltpu.VMEM((STEPS, 2, 4, rows + 2 * COST_HALO, lanes), f32),
                pltpu.VMEM((2, rows, lanes), f32),
                pltpu.VMEM((STEPS, 2, 8, lanes), f32),
                pltpu.VMEM((nx, 1, lanes), f32),
                pltpu.VMEM((ny, 1, lanes), f32),
                pltpu.SemaphoreType.DMA((8,)),
                pltpu.SemaphoreType.DMA((28,)),
                pltpu.SemaphoreType.DMA((28,)),
                pltpu.SemaphoreType.DMA((nx + ny,)),
                pltpu.SemaphoreType.DMA((nx,)),
                pltpu.SemaphoreType.DMA((ny,)),
            ],
            compiler_params=pltpu.CompilerParams(
                collective_id=0, has_side_effects=True, vmem_limit_bytes=32 * 1024 * 1024
            ),
        )(start, vel, sts, wind, strength, mass, land, region, obs)
        return pl.pallas_call(
            split_kernel,
            out_shape=(
                jax.ShapeDtypeStruct((5, rows, lanes), f32),
                jax.ShapeDtypeStruct((2, rows, lanes), f32),
            ),
            in_specs=[vm],
            out_specs=(hbm, hbm),
            scratch_shapes=[pltpu.SemaphoreType.DMA((2,))],
        )(pltpu.with_memory_space_constraint(both, pltpu.VMEM))

    block = P(None, "gy", "gx")
    flat = P("gy", "gx")
    return jax.shard_map(
        per_device,
        mesh=mesh,
        in_specs=(block, block, block, flat, flat, flat, flat, block, P()),
        out_specs=(block, block),
        check_vma=False,
    )
```
